32 devices in a mesh: ctx: 4 (over z), tp: 4 (over y, core), ep: 2 (over x).
Axes of the slice: x: 2, y: 2, z: 4, core: 2. Of those that a mesh axis runs over, the one named last changes fastest.
Arguments:
- resid: bfloat16 [1024, 6144], P('ctx', ('tp', 'ep')), may hold values from -60 to 60
- queries: bfloat16 [1024, 6144], P('ctx', 'tp'), may hold values from -6 to 6
- keys: bfloat16 [1024, 1024], P('ctx', 'tp'), may hold values from -4 to 4
- values: bfloat16 [1024, 1024], P('ctx', 'tp'), may hold values from -5 to 5
- w_out: bfloat16 [6144, 6144], P('tp', ('ctx', 'ep')), may hold values from -0.078125 to 0.078125
- norm_gain: bfloat16 [6144], P(('tp', 'ep')), may hold values from 0.5 to 1.5
- w_gate: bfloat16 [4, 6144, 8192], P('tp', None, ('ctx', 'ep')), may hold values from -0.078125 to 0.078125
- w_up: bfloat16 [4, 6144, 8192], P('tp', None, ('ctx', 'ep')), may hold values from -0.078125 to 0.078125
- w_down: bfloat16 [4, 8192, 6144], P('tp', ('ctx', 'ep')), may hold values from -0.0625 to 0.0625
- expert_ids: int32 [1024, 2], P('ctx'), may hold values from 0 to 3, all different within a row; in each aligned block of 256 rows (0 to 255, 256 to 511, ...) at most 192 rows name the same one
- route_units: int32 [1024, 2], P('ctx'), may hold values from 1 to 65535
Outputs:
- mixed: bfloat16 [1024, 6144], P('ctx', ('tp', 'ep'))
The draws below stay inside these ranges and needn't reach their ends.
Inputs may be any that keep to these rules, and one draw needn't show every extreme that they name: `expert_ids`: each row names two different experts; in every aligned block of 256 rows no expert is named by more than 192 rows, a bound that some block reaches.
All inputs are finite; a program needn't handle non-finite values.
Results may differ from the reference program's by a relative error of at most 0.01.
Values may be sent and summed in bfloat16 or wider, within the bound.
A program may use at most 128 MiB of HBM per device.

```python
import math
import jax
import jax.numpy as jnp
import numpy as np
from jax import lax

D = 6144
H = 48
KVH = 8
HD = 128
FF = 8192
TOK_DEV = 256
TOKENS = 1024
EXPERTS = 4
CAP = 192
N_CTX = 4


def draw_resid(key, part):
    base = jax.random.fold_in(key, 5)
    key_z, key_rows, key_cols = jax.random.split(base, 3)
    column = jnp.arange(D, dtype=jnp.float32) / D
    values_z = jnp.clip(jax.random.normal(key_z, (TOKENS, D), jnp.float32), -4.0, 4.0)
    row_scale = jnp.power(10.0, jax.random.uniform(key_rows, (TOKENS, 1), jnp.float32, -0.5, 0.5))
    col_scale = jnp.power(10.0, jax.random.uniform(key_cols, (1, D), jnp.float32, -0.5, 0.5)) * jnp.power(3.0, 0.5 * (column - 0.5))[None, :]
    return (values_z * row_scale * col_scale).astype(jnp.bfloat16)


def query_key_pair(key):
    base = jax.random.fold_in(key, 17)
    key_q, key_k = jax.random.split(base, 2)
    query_vals = jnp.clip(jax.random.normal(key_q, (TOKENS, H, HD), jnp.float32), -4.0, 4.0)
    key_vals = jnp.clip(jax.random.normal(key_k, (TOKENS, KVH, HD), jnp.float32), -4.0, 4.0)
    return (query_vals.reshape(TOKENS, H * HD), key_vals.reshape(TOKENS, KVH * HD))


def draw_queries(key, part):
    return query_key_pair(key)[0].astype(jnp.bfloat16)


def draw_keys(key, part):
    return query_key_pair(key)[1].astype(jnp.bfloat16)


def touch_ends(drawn, stream_key, low, high):
    longest = drawn.shape.index(max(drawn.shape))
    spots = []
    for shift in (0, 1):
        where = [jax.random.randint(jax.random.fold_in(stream_key, axis), (), 0, length) for axis, length in enumerate(drawn.shape)]
        where[longest] = (where[longest] + shift) % drawn.shape[longest]
        spots.append(tuple(where))
    return drawn.at[spots[0]].set(low).at[spots[1]].set(high)


def levels(key, extent, cuts, least, high):
    gain = 1.0
    for position, shards_of in cuts:
        heights = jax.random.uniform(jax.random.fold_in(jax.random.fold_in(key, 6), position), (shards_of,), jnp.float32, least / len(cuts), high / len(cuts))
        gain = gain * jnp.repeat(jnp.exp(heights), extent[position] // shards_of).reshape((-1,) + (1,) * (len(extent) - 1 - position))
    return gain


def deal_out(rng, own, number, rows, count, top, limit, skew):
    ranking = jax.random.permutation(rng, count)
    crowded, common = portions_of(count, rows * top, limit, skew, True), portions_of(count, rows * top, limit, skew, False)
    places = jnp.arange(count)

    def named(sizes, offset_by):
        used = int((sizes > 0).sum())
        fixed = max(1, used // 4)
        passed = fixed + (places - fixed + offset_by * (used - fixed)) % max(1, count - fixed)
        return jnp.zeros((count,), jnp.int32).at[ranking[jnp.where(places < fixed, places, passed)]].set(jnp.asarray(sizes, jnp.int32))

    sizes = jnp.where(number % 4 == 0, named(crowded, number // 4), named(common, number - number // 4 - 1))
    mixed = jax.random.permutation(jax.random.fold_in(own, 3), count)
    giver, receiver = mixed[0:count // 2 * 2:2], mixed[1:count // 2 * 2:2]
    slack = jnp.minimum(sizes[giver] - 1, limit - sizes[receiver]) // 2
    slack = jnp.where((giver == ranking[0]) | (receiver == ranking[0]) | (sizes[receiver] == 0), 0, jnp.maximum(slack, 0))
    passed = jax.random.randint(jax.random.fold_in(own, 4), (count // 2,), 0, 1 << 20) % (slack + 1)
    sizes = sizes.at[giver].add(-passed).at[receiver].add(passed)
    labels = jnp.searchsorted(jnp.cumsum(sizes), jnp.arange(rows * top), side="right").astype(jnp.int32)
    grid = labels.reshape(top, rows).T
    grid = grid[jax.random.permutation(jax.random.fold_in(own, 1), rows)]
    offset_by = jax.random.randint(jax.random.fold_in(own, 2), (rows, 1), 0, top)
    return jnp.take_along_axis(grid, (jnp.arange(top)[None, :] + offset_by) % top, axis=1)


def portions_of(amount, total, limit, lean, full):
    weights = [(1 << 20) // math.isqrt(grade ** lean) + 1 for grade in range(1, amount + 1)]
    largest = limit if full else min(limit, max(-(-total // amount), total * weights[0] // sum(weights)))
    least = 1 if total - largest >= amount - 1 else 0
    counts, rest = [largest] + [least] * (amount - 1), total - largest - least * (amount - 1)
    while rest > 0:
        free = [i for i in range(1, amount) if counts[i] < largest] or [i for i in range(1, amount) if counts[i] < limit]
        whole, left = sum([weights[i] for i in free]), rest
        for i in free:
            more = min(limit - counts[i], max(1, left * weights[i] // whole), rest)
            counts[i] = counts[i] + more
            rest = rest - more
    return np.array(counts)


def gaussian(own_key, extent, spread, limit, shards=(), kind=jnp.bfloat16):
    loudness = levels(own_key, extent, shards, -0.22, 0.18) if shards else 1.0
    values = jax.random.normal(own_key, extent, jnp.float32) * spread * loudness
    return jnp.minimum(jnp.maximum(values, -limit), limit).astype(kind)


def setup_inputs(seed: int = 0) -> dict:
    splits = jax.random.split(jax.random.key(seed), 12)
    resid = draw_resid(jax.random.fold_in(splits[11], 71), 0)
    queries = draw_queries(jax.random.fold_in(splits[11], 71), 0)
    keys = draw_keys(jax.random.fold_in(splits[11], 71), 0)
    values = gaussian(splits[3], (TOKENS, KVH * HD), 1.0, 5.0, ((0, 4), (1, 4)))
    w_out = gaussian(splits[4], (H * HD, D), (H * HD) ** -0.5, 0.078125, ((0, 4), (1, 8)))
    norm_gain = jnp.clip(1.0 + 0.1 * jax.random.normal(splits[5], (D,), jnp.float32), 0.5, 1.5).astype(jnp.bfloat16)
    w_gate = gaussian(splits[6], (EXPERTS, D, FF), D ** -0.5, 0.078125, ((0, 4), (2, 8)))
    w_up = gaussian(splits[7], (EXPERTS, D, FF), D ** -0.5, 0.078125, ((0, 4), (2, 8)))
    w_down = gaussian(splits[8], (EXPERTS, FF, D), FF ** -0.5, 0.0625, ((0, 4), (1, 8)))
    expert_ids_keys = jax.random.split(jax.random.fold_in(splits[9], 1), TOKENS // TOK_DEV)
    expert_ids_turns = jax.random.permutation(jax.random.fold_in(splits[9], 3), TOKENS // TOK_DEV)
    expert_ids = jax.vmap(lambda own, number: deal_out(jax.random.fold_in(splits[9], 2), own, number, TOK_DEV, EXPERTS, 2, CAP, 2))(expert_ids_keys, expert_ids_turns).reshape((TOKENS, 2))
    route_units = touch_ends(jax.random.randint(splits[10], (TOKENS, 2), 1, 65536), jax.random.fold_in(splits[10], 1), 1, 65535).astype(jnp.int32)
    return dict(resid=resid, queries=queries, keys=keys, values=values, w_out=w_out, norm_gain=norm_gain, w_gate=w_gate, w_up=w_up, w_down=w_down, expert_ids=expert_ids, route_units=route_units)


def attend(query_group, key_group, value_group):
    positions = jnp.arange(TOKENS, dtype=jnp.int32)
    causal = positions[None, :] <= positions[:, None]
    scores = jnp.einsum('tgd,nd->gtn', query_group.astype(jnp.float32), key_group.astype(jnp.float32)) * HD ** (-0.5)
    scores = jnp.where(causal[None], scores, -jnp.inf)
    row_max = lax.optimization_barrier(jnp.max(scores, axis=-1, keepdims=True))
    probs = jnp.where(causal[None], jnp.exp(scores - row_max), 0.0)
    denom = lax.optimization_barrier(jnp.sum(probs, axis=-1))
    probs_b = probs.astype(jnp.bfloat16)
    weighted = jnp.einsum('gtn,nd->gtd', probs_b.astype(jnp.float32), value_group.astype(jnp.float32))
    return weighted / denom[..., None]

def run_expert(operands):
    expert_in, gate_w, up_w, down_w = operands
    flat = expert_in.reshape(N_CTX * CAP, D)
    gate = jnp.dot(flat, gate_w, preferred_element_type=jnp.float32)
    upper = jnp.dot(flat, up_w, preferred_element_type=jnp.float32)
    hidden = (jax.nn.silu(gate) * upper).astype(jnp.bfloat16)
    result = jnp.dot(hidden, down_w, preferred_element_type=jnp.float32).astype(jnp.bfloat16)
    return result.reshape(N_CTX, CAP, D)

def reference(resid, queries, keys, values, w_out, norm_gain, w_gate, w_up, w_down, expert_ids, route_units):
    group = H // KVH
    query_heads = queries.reshape(TOKENS, KVH, group, HD).transpose(1, 0, 2, 3)
    key_heads = keys.reshape(TOKENS, KVH, HD).transpose(1, 0, 2)
    value_heads = values.reshape(TOKENS, KVH, HD).transpose(1, 0, 2)
    heads_out = lax.map(lambda ops: attend(ops[0], ops[1], ops[2]), (query_heads, key_heads, value_heads))
    attn = heads_out.transpose(2, 0, 1, 3).reshape(TOKENS, H * HD).astype(jnp.bfloat16)
    proj = jnp.dot(attn, w_out, preferred_element_type=jnp.float32)
    hres = (resid.astype(jnp.float32) + proj).astype(jnp.bfloat16)
    hfloat = hres.astype(jnp.float32)
    mean_sq = lax.optimization_barrier(jnp.mean(hfloat * hfloat, axis=1, keepdims=True))
    normed = (hfloat * lax.rsqrt(mean_sq + 1e-05) * norm_gain.astype(jnp.float32)).astype(jnp.bfloat16)
    ids = expert_ids.reshape(N_CTX, TOK_DEV, 2)
    onehot = (ids[..., None] == jnp.arange(EXPERTS, dtype=jnp.int32)).astype(jnp.int32)
    per_token = lax.optimization_barrier(jnp.sum(onehot, axis=2))
    earlier = jnp.cumsum(per_token, axis=1) - per_token
    slot = lax.optimization_barrier(jnp.sum(onehot * earlier[:, :, None, :], axis=-1)).astype(jnp.int32)
    block = jnp.broadcast_to(jnp.arange(N_CTX, dtype=jnp.int32)[:, None, None], ids.shape)
    rows = jnp.broadcast_to(normed.reshape(N_CTX, TOK_DEV, 1, D), (N_CTX, TOK_DEV, 2, D))
    expert_in = jnp.zeros((EXPERTS, N_CTX, CAP, D), jnp.bfloat16).at[ids, block, slot].set(rows)
    expert_out = lax.map(run_expert, (expert_in, w_gate, w_up, w_down))
    picked = expert_out[ids, block, slot]
    units = route_units.astype(jnp.float32).reshape(N_CTX, TOK_DEV, 2)
    weights = (units / lax.optimization_barrier(jnp.sum(units, axis=-1, keepdims=True))).astype(jnp.bfloat16)
    moe = lax.optimization_barrier(jnp.sum(weights.astype(jnp.float32)[..., None] * picked.astype(jnp.float32), axis=2))
    return (hfloat + moe.reshape(TOKENS, D)).astype(jnp.bfloat16)
```

```python
import jax
import jax.numpy as jnp
from jax import lax
from jax.sharding import PartitionSpec as P

D = 6144
HD = 128


def from_partner(x, axis, distance):
    return lax.ppermute(x, axis, [(i, i ^ 1 << distance) for i in range(lax.axis_size(axis))])


def columns_of(w, parity, part, width, feat_dev, tp_size, ep_size):
    return jnp.concatenate(
        [
            lax.dynamic_slice_in_dim(w, (t * ep_size + parity) * feat_dev + part * width, width, 1)
            for t in range(tp_size)
        ],
        axis=1,
    )


def on_device(
    resid, queries, keys, values, w_out, norm_gain, w_gate, w_up, w_down, expert_ids, route_units
):
    tp_size = lax.axis_size("tp")
    ep_size = lax.axis_size("ep")
    ctx_size = lax.axis_size("ctx")
    me_tp = lax.axis_index("tp")
    parity = lax.axis_index("ep")
    tok_rows = queries.shape[0]
    heads_dev = queries.shape[1] // HD
    kv_dev = keys.shape[1] // HD
    group = heads_dev // kv_dev
    feat_dev = resid.shape[1]
    hidden_dev = w_gate.shape[2]
    features = w_gate.shape[1]
    capacity = 3 * tok_rows // tp_size
    parts = 2 if feat_dev % 256 == 0 else 1
    width = feat_dev // parts

    give = [
        columns_of(w_down[0], 1 - parity, q, width, feat_dev, tp_size, ep_size)
        for q in range(parts)
    ]
    queries, *give = lax.optimization_barrier((queries, *give))
    got_cols = [from_partner(g, "ep", 0) for g in give]
    mine_cols = [
        columns_of(w_down[0], parity, q, width, feat_dev, tp_size, ep_size) for q in range(parts)
    ]

    first_pos = lax.axis_index("ctx") * tok_rows
    query_heads = queries.reshape(tok_rows, kv_dev, group, HD)
    query_pos = first_pos + jnp.arange(tok_rows, dtype=jnp.int32)
    both = lax.all_gather(jnp.concatenate([keys, values], axis=1), "ctx", axis=0, tiled=True)
    count = both.shape[0]
    key_rows = both[:, : kv_dev * HD].reshape(count, kv_dev, HD)
    value_rows = both[:, kv_dev * HD :].reshape(count, kv_dev, HD)
    scores = jnp.einsum(
        "tkgd,nkd->kgtn", query_heads, key_rows, preferred_element_type=jnp.float32
    ) * HD ** (-0.5)
    key_pos = jnp.arange(count, dtype=jnp.int32)
    allowed = (key_pos[None, :] <= query_pos[:, None])[None, None]
    row_max = jnp.max(jnp.where(allowed, scores, -1e30), axis=-1)
    probs = jnp.where(allowed, jnp.exp(scores - row_max[..., None]), 0.0)
    denom = jnp.sum(probs, axis=-1)
    probs_b = probs.astype(jnp.bfloat16)
    update = jnp.einsum("kgtn,nkd->kgtd", probs_b, value_rows, preferred_element_type=jnp.float32)
    attn = (
        (update / denom[..., None])
        .transpose(2, 0, 1, 3)
        .reshape(tok_rows, heads_dev * HD)
        .astype(jnp.bfloat16)
    )

    attn_all = lax.all_gather(attn, "ctx", axis=0, tiled=True)
    partial_proj = jnp.dot(attn_all, w_out, preferred_element_type=jnp.float32)
    block = lax.psum_scatter(
        partial_proj.astype(jnp.bfloat16), "tp", scatter_dimension=0, tiled=True
    )
    block, *cols = lax.optimization_barrier((block, *got_cols, *mine_cols))
    got_cols, mine_cols = cols[:parts], cols[parts:]
    swap = [
        (c * tp_size + t, t * tp_size + c) for c in range(ctx_size) for t in range(tp_size)
    ]
    proj = lax.ppermute(block, ("ctx", "tp"), swap).astype(jnp.float32)
    hres = (resid.astype(jnp.float32) + proj).astype(jnp.bfloat16)
    hfloat = hres.astype(jnp.float32)

    own = lax.all_gather(hres, "ctx", axis=0, tiled=False)
    squares = lax.all_gather(jnp.sum(hfloat * hfloat, axis=1), ("ctx", "tp", "ep"), axis=0)
    square_total = jnp.sum(squares.reshape(ctx_size, tp_size * ep_size, tok_rows), axis=1)
    scale = lax.rsqrt(square_total / D + 1e-05)[:, :, None]
    gain_all = lax.all_gather(norm_gain, ("tp", "ep"), axis=0, tiled=True)
    side = from_partner(own, "ep", 0)
    half = ctx_size // 2
    blocks = [(me_tp, parity, own), (me_tp, 1 - parity, side)]
    for k in range(1, tp_size // 2):
        turn = [(i, (i + 2 * k) % tp_size) for i in range(tp_size)]
        origin = (me_tp + tp_size - 2 * k) % tp_size
        far = lax.ppermute(own, "tp", turn)
        far_a = lax.ppermute(side[:half], "tp", turn)
        far_b = from_partner(far[half:], "ep", 0)
        blocks.append((origin, parity, far))
        blocks.append((origin, 1 - parity, jnp.concatenate([far_a, far_b], axis=0)))
    blocks = blocks + [(t ^ 1, e, from_partner(h, "tp", 0)) for t, e, h in blocks]

    ids_all = lax.all_gather(expert_ids, "ctx", axis=0, tiled=False)
    named = jnp.any(ids_all == me_tp, axis=-1)
    named_i = named.astype(jnp.int32)
    slot_all = jnp.cumsum(named_i, axis=1) - named_i
    picks = (
        named[:, None, :]
        & (slot_all[:, None, :] == jnp.arange(capacity, dtype=jnp.int32)[None, :, None])
    ).astype(jnp.bfloat16)
    expert_in = jnp.zeros((ctx_size * capacity, features), jnp.bfloat16)
    for t, e, h in blocks:
        at = (t * ep_size + e) * feat_dev
        gain = lax.dynamic_slice_in_dim(gain_all, at, feat_dev, 0).astype(jnp.float32)
        normed = (h.astype(jnp.float32) * scale * gain).astype(jnp.bfloat16)
        rows = jnp.einsum("csn,cnj->csj", picks, normed, preferred_element_type=jnp.float32)
        expert_in = lax.dynamic_update_slice(
            expert_in, rows.astype(jnp.bfloat16).reshape(ctx_size * capacity, feat_dev), (0, at)
        )

    pieces = 2
    hid = hidden_dev // pieces
    mine, got = [], []
    for i in range(pieces):
        cols = slice(i * hid, (i + 1) * hid)
        gate = jnp.dot(expert_in, w_gate[0][:, cols], preferred_element_type=jnp.float32)
        upper = jnp.dot(expert_in, w_up[0][:, cols], preferred_element_type=jnp.float32)
        mine.append((jax.nn.silu(gate) * upper).astype(jnp.bfloat16))
        got.append(from_partner(mine[-1], "ep", 0))
    hidden_both = jnp.concatenate(mine + got, axis=1)

    onehot = (expert_ids[..., None] == jnp.arange(tp_size, dtype=jnp.int32)).astype(jnp.int32)
    per_token = jnp.sum(onehot, axis=1)
    earlier = jnp.cumsum(per_token, axis=0) - per_token
    slot = jnp.sum(onehot * earlier[:, None, :], axis=-1)
    codes = expert_ids * capacity + slot
    slot_ids = jnp.arange(tp_size * capacity, dtype=jnp.int32)
    units = route_units.astype(jnp.float32)
    weights = (units / jnp.sum(units, axis=-1, keepdims=True)).astype(jnp.bfloat16)
    combine = jnp.where(slot_ids[None, :] == codes[:, 0:1], weights[:, 0:1], 0.0) + jnp.where(
        slot_ids[None, :] == codes[:, 1:2], weights[:, 1:2], 0.0
    )
    outs = []
    for q in range(parts):
        product = jnp.dot(
            hidden_both,
            jnp.concatenate([mine_cols[q], got_cols[q]], axis=0),
            preferred_element_type=jnp.float32,
        )
        expert_sum = lax.psum_scatter(
            product.astype(jnp.bfloat16), "ctx", scatter_dimension=0, tiled=True
        )
        returned = lax.all_to_all(expert_sum, "tp", split_axis=1, concat_axis=0, tiled=True)
        moe = jnp.dot(combine, returned, preferred_element_type=jnp.float32)
        outs.append((hfloat[:, q * width : (q + 1) * width] + moe).astype(jnp.bfloat16))
    return jnp.concatenate(outs, axis=1)


def solution(mesh):
    placed = (
        P("ctx", ("tp", "ep")),
        P("ctx", "tp"),
        P("ctx", "tp"),
        P("ctx", "tp"),
        P("tp", ("ctx", "ep")),
        P(("tp", "ep")),
        P("tp", None, ("ctx", "ep")),
        P("tp", None, ("ctx", "ep")),
        P("tp", ("ctx", "ep"), None),
        P("ctx", None),
        P("ctx", None),
    )
    return jax.shard_map(
        on_device, mesh=mesh, in_specs=placed, out_specs=P("ctx", ("tp", "ep")), check_vma=False
    )
```
